32 devices in a mesh: dp: 8 (over z, y), sy: 2 (over x), sx: 2 (over core).
Axes of the slice: x: 2, y: 2, z: 4, core: 2. Of those that a mesh axis runs over, the one named last changes fastest.
Arguments:
- features: bfloat16 [8, 56, 56, 256], P('dp', 'sy', 'sx'), may hold values from -8 to 8
- labels: int32 [8], P('dp'), may hold values from 0 to 999
- grid: int32 [2], replicated, may hold values from 0 to 49
- w_reduce: bfloat16 [3, 256, 64], P(None, None, 'dp'), may hold values from -0.375 to 0.375
- w_spatial: bfloat16 [3, 3, 3, 64, 64], P(None, None, None, None, 'dp'), may hold values from -0.25 to 0.25
- w_expand: bfloat16 [3, 64, 256], P(None, None, 'dp'), may hold values from -0.75 to 0.75
- w_class: bfloat16 [256, 1000], P('dp'), may hold values from -1.5 to 1.5
- dir_reduce: bfloat16 [2, 3, 256, 64], P(None, None, None, 'dp'), may hold values from -6 to 6
- dir_spatial: bfloat16 [2, 3, 3, 3, 64, 64], P(None, None, None, None, None, 'dp'), may hold values from -6 to 6
- dir_expand: bfloat16 [2, 3, 64, 256], P(None, None, None, 'dp'), may hold values from -6 to 6
- dir_class: bfloat16 [2, 256, 1000], P(None, 'dp'), may hold values from -6 to 6
- gain_mid: float32 [3, 2, 64], replicated, may hold values from 0.5 to 1.5
- shift_mid: float32 [3, 2, 64], replicated, may hold values from -3 to 3
- gain_out: float32 [3, 256], replicated, may hold values from 0.5 to 1.5
- shift_out: float32 [3, 256], replicated, may hold values from -3 to 3
Outputs:
- section_out: bfloat16 [8, 56, 56, 256], P('dp', 'sy', 'sx')
- image_loss: float32 [8], P('dp')
- mean_loss: float32 [], replicated
The draws below stay inside these ranges and needn't reach their ends.
All inputs are finite; a program needn't handle non-finite values.
Results may differ from the reference program's by a relative error of at most 0.012.
Values may be sent and summed in bfloat16 or wider, within the bound.
A program may use at most 64 MiB of HBM per device.

```python
import jax
import jax.numpy as jnp
from jax import lax

FEAT = 256
MID = 64
CLASSES = 1000
BLOCKS = 3
GRID = 50
IMAGES = 8
SIDE_H = 56
SIDE_W = 56


def draw_features(key, part):
    key_mean = jax.random.fold_in(key, 11)
    key_noise = jax.random.fold_in(key, 12)
    key_level = jax.random.fold_in(key, 14)
    key_spread = jax.random.fold_in(key, 15)
    key_amount = jax.random.fold_in(key, 16)
    key_tilt = jax.random.fold_in(key, 17)
    row_index = jnp.arange(SIDE_H, dtype=jnp.int32)
    col_index = jnp.arange(SIDE_W, dtype=jnp.int32)
    upper = jnp.where(row_index < SIDE_H // 2, 1.0, -1.0).astype(jnp.float32)
    leftside = jnp.where(col_index < SIDE_W // 2, 1.0, -1.0).astype(jnp.float32)
    quadrant = upper[:, None] * leftside[None, :]
    level = jax.random.uniform(key_level, (IMAGES,), jnp.float32, 0.5, 2.0)
    spread = jax.random.uniform(key_spread, (IMAGES,), jnp.float32, 0.35, 1.75)
    amount = jax.random.uniform(key_amount, (IMAGES,), jnp.float32, 0.5, 1.1)
    pattern = jax.random.normal(key_mean, (FEAT,), jnp.float32)
    tilt = jax.random.normal(key_tilt, (FEAT,), jnp.float32)
    noise = jax.random.normal(key_noise, (IMAGES, SIDE_H, SIDE_W, FEAT), jnp.float32)
    value = level[:, None, None, None] * pattern[None, None, None, :]
    value = value + 0.8 * amount[:, None, None, None] * quadrant[None, :, :, None] * tilt[None, None, None, :]
    value = value + spread[:, None, None, None] * noise
    return jnp.clip(value, -8.0, 8.0).astype(jnp.bfloat16)


def plant(result, key, low, largest):
    index_at = [jax.random.randint(jax.random.fold_in(key, axis), (), 0, length) for axis, length in enumerate(result.shape)]
    main_axis = result.shape.index(max(result.shape))
    neighbour = index_at[:main_axis] + [(index_at[main_axis] + 1) % result.shape[main_axis]] + index_at[main_axis + 1:]
    return result.at[tuple(index_at)].set(low).at[tuple(neighbour)].set(largest)


def shard_levels(stream_key, dims, pieces, low, largest):
    level = 1.0
    for axis_at, shards_of in pieces:
        draws = jax.random.uniform(jax.random.fold_in(jax.random.fold_in(stream_key, 6), axis_at), (shards_of,), jnp.float32, low / len(pieces), largest / len(pieces))
        level = level * jnp.repeat(jnp.exp(draws), dims[axis_at] // shards_of).reshape((-1,) + (1,) * (len(dims) - 1 - axis_at))
    return level


def normal_values(key, extent, scale, reach, shards=(), kind=jnp.bfloat16):
    loudness = shard_levels(key, extent, shards, -0.22, 0.18) if shards else 1.0
    array = jax.random.normal(key, extent, jnp.float32) * scale * loudness
    return jnp.minimum(jnp.maximum(array, -reach), reach).astype(kind)


def setup_inputs(seed: int = 0) -> dict:
    splits = jax.random.split(jax.random.key(seed), 16)
    features = draw_features(jax.random.fold_in(splits[15], 71), 0)
    labels = plant(jax.random.randint(splits[1], (IMAGES,), 0, CLASSES), jax.random.fold_in(splits[1], 1), 0, CLASSES - 1).astype(jnp.int32)
    grid = jax.random.randint(splits[2], (2,), 0, GRID).astype(jnp.int32)
    w_reduce = normal_values(splits[3], (BLOCKS, FEAT, MID), FEAT ** -0.5, 0.375, ((2, 8),))
    w_spatial = normal_values(splits[4], (BLOCKS, 3, 3, MID, MID), (9 * MID) ** -0.5, 0.25, ((4, 8),))
    w_expand = normal_values(splits[5], (BLOCKS, MID, FEAT), MID ** -0.5, 0.75, ((2, 8),))
    w_class = normal_values(splits[6], (FEAT, CLASSES), (FEAT // 16) ** -0.5, 1.5, ((0, 8),))
    dir_reduce = normal_values(splits[7], (2, BLOCKS, FEAT, MID), 1.0, 6.0, ((3, 8),))
    dir_spatial = normal_values(splits[8], (2, BLOCKS, 3, 3, MID, MID), 1.0, 6.0, ((5, 8),))
    dir_expand = normal_values(splits[9], (2, BLOCKS, MID, FEAT), 1.0, 6.0, ((3, 8),))
    dir_class = normal_values(splits[10], (2, FEAT, CLASSES), 1.0, 6.0, ((1, 8),))
    gain_mid = jnp.clip(1.0 + 0.1 * jax.random.normal(splits[11], (BLOCKS, 2, MID), jnp.float32), 0.5, 1.5)
    shift_mid = normal_values(splits[12], (BLOCKS, 2, MID), 0.5, 3.0, (), jnp.float32)
    gain_out = jnp.clip(1.0 + 0.1 * jax.random.normal(splits[13], (BLOCKS, FEAT), jnp.float32), 0.5, 1.5)
    shift_out = normal_values(splits[14], (BLOCKS, FEAT), 0.5, 3.0, (), jnp.float32)
    return {"features": features, "labels": labels, "grid": grid, "w_reduce": w_reduce, "w_spatial": w_spatial, "w_expand": w_expand, "w_class": w_class, "dir_reduce": dir_reduce, "dir_spatial": dir_spatial, "dir_expand": dir_expand, "dir_class": dir_class, "gain_mid": gain_mid, "shift_mid": shift_mid, "gain_out": gain_out, "shift_out": shift_out}


EPS_NORM = 1e-06
EPS_BN = 1e-05

def coefficients(grid):
    values = grid.astype(jnp.float32)
    alpha = (2.0 * values + 1.0 - GRID) / GRID
    return (alpha[0], alpha[1])

def filter_ratio(base, direction, axes):
    base_norm = jnp.sqrt(lax.optimization_barrier(jnp.sum(jnp.square(base.astype(jnp.float32)), axis=axes, keepdims=True)))
    dir_norm = jnp.sqrt(lax.optimization_barrier(jnp.sum(jnp.square(direction.astype(jnp.float32)), axis=axes, keepdims=True)) + EPS_NORM)
    return base_norm / dir_norm

def perturb(base, dir_a, dir_b, axes, alpha_a, alpha_b):
    ratio_a = filter_ratio(base, dir_a, axes)
    ratio_b = filter_ratio(base, dir_b, axes)
    value = base.astype(jnp.float32) + alpha_a * ratio_a * dir_a.astype(jnp.float32) + alpha_b * ratio_b * dir_b.astype(jnp.float32)
    return value.astype(jnp.bfloat16)

def batch_norm(y, gain, shift):
    axes = (0, 1, 2)
    mean = lax.optimization_barrier(jnp.mean(y, axis=axes))
    centred = y - mean
    var = lax.optimization_barrier(jnp.mean(centred * centred, axis=axes))
    return centred * lax.rsqrt(var + EPS_BN) * gain + shift

def pointwise(x, weight):
    shape = x.shape
    flat = jnp.dot(x.reshape(-1, shape[-1]), weight, preferred_element_type=jnp.float32)
    return flat.reshape(shape[:-1] + (weight.shape[-1],))

def reference(features, labels, grid, w_reduce, w_spatial, w_expand, w_class, dir_reduce, dir_spatial, dir_expand, dir_class, gain_mid, shift_mid, gain_out, shift_out):
    alpha_a, alpha_b = coefficients(grid)
    current = features
    for block in range(BLOCKS):
        p_reduce = perturb(w_reduce[block], dir_reduce[0, block], dir_reduce[1, block], (0,), alpha_a, alpha_b)
        p_spatial = perturb(w_spatial[block], dir_spatial[0, block], dir_spatial[1, block], (0, 1, 2), alpha_a, alpha_b)
        p_expand = perturb(w_expand[block], dir_expand[0, block], dir_expand[1, block], (0,), alpha_a, alpha_b)
        first = pointwise(current, p_reduce)
        first = jax.nn.relu(batch_norm(first, gain_mid[block, 0], shift_mid[block, 0])).astype(jnp.bfloat16)
        second = lax.conv_general_dilated(first, p_spatial, (1, 1), 'SAME', dimension_numbers=('NHWC', 'HWIO', 'NHWC'), preferred_element_type=jnp.float32)
        second = jax.nn.relu(batch_norm(second, gain_mid[block, 1], shift_mid[block, 1])).astype(jnp.bfloat16)
        third = batch_norm(pointwise(second, p_expand), gain_out[block], shift_out[block])
        current = jax.nn.relu(current.astype(jnp.float32) + third).astype(jnp.bfloat16)
    pooled = (lax.optimization_barrier(jnp.sum(current.astype(jnp.float32), axis=(1, 2))) / (SIDE_H * SIDE_W)).astype(jnp.bfloat16)
    p_class = perturb(w_class, dir_class[0], dir_class[1], (0,), alpha_a, alpha_b)
    logits = jnp.dot(pooled, p_class, preferred_element_type=jnp.float32)
    total = jnp.log(lax.optimization_barrier(jnp.sum(jnp.exp(logits), axis=1)))
    classes = lax.broadcasted_iota(jnp.int32, logits.shape, 1)
    picked = lax.optimization_barrier(jnp.sum(jnp.where(classes == labels[:, None], logits, 0.0), axis=1))
    image_loss = total - picked
    mean_loss = jnp.sum(image_loss) / IMAGES
    return (current, image_loss, mean_loss)
```

```python
import functools

import jax
import jax.numpy as jnp
from jax import lax
from jax.experimental import pallas as pl
from jax.experimental.pallas import tpu as pltpu
from jax.sharding import PartitionSpec as P

BLOCKS = 3
GRID = 50


EPS_NORM = 1e-06
EPS_BN = 1e-05


def extended(cells, sides, width):
    for axis, dim in sides:
        count = lax.axis_size(axis)
        ends = count - 1
        head = lax.slice_in_dim(cells, 0, width, axis=dim)
        tail = lax.slice_in_dim(cells, cells.shape[dim] - width, cells.shape[dim], axis=dim)
        cells = jnp.concatenate(
            [
                lax.ppermute(tail, axis, [(i, (i + 1) % count) for i in range(ends)]),
                cells,
                lax.ppermute(head, axis, [((i + 1) % count, i) for i in range(ends)]),
            ],
            axis=dim,
        )
    return cells


def coefficients(grid):
    values = grid.astype(jnp.float32)
    alpha = (2.0 * values + 1.0 - GRID) / GRID
    return (alpha[0], alpha[1])


def filter_ratio(base, direction):
    base_norm = jnp.sqrt(jnp.sum(jnp.square(base.astype(jnp.float32)), axis=0, keepdims=True))
    dir_norm = jnp.sqrt(
        jnp.sum(jnp.square(direction.astype(jnp.float32)), axis=0, keepdims=True) + EPS_NORM
    )
    return base_norm / dir_norm


def combine_filters(base, dir_a, dir_b, alpha_a, alpha_b):
    ratio_a = filter_ratio(base, dir_a)
    ratio_b = filter_ratio(base, dir_b)
    value = (
        base.astype(jnp.float32)
        + alpha_a * ratio_a * dir_a.astype(jnp.float32)
        + alpha_b * ratio_b * dir_b.astype(jnp.float32)
    )
    return value.astype(jnp.bfloat16)


def perturbed_product(left, base, dir_a, dir_b, alpha_a, alpha_b):
    local = combine_filters(base, dir_a, dir_b, alpha_a, alpha_b)
    return jnp.dot(
        left, lax.all_gather(local, "dp", axis=1, tiled=True), preferred_element_type=jnp.float32
    )


def normalize(y, gain, shift, count):
    mean = lax.psum(jnp.sum(y, axis=0), ("dp", "sy", "sx")) / count
    centred = y - mean
    var = lax.psum(jnp.sum(centred * centred, axis=0), ("dp", "sy", "sx")) / count
    return centred * lax.rsqrt(var + EPS_BN) * gain + shift


def padded_tile(inner):
    return extended(inner, (("sy", 1), ("sx", 2)), 1)


def per_device(
    features,
    labels,
    grid,
    w_reduce,
    w_spatial,
    w_expand,
    w_class,
    dir_reduce,
    dir_spatial,
    dir_expand,
    dir_class,
    gain_mid,
    shift_mid,
    gain_out,
    shift_out,
):
    alpha_a, alpha_b = coefficients(grid)
    images, rows, cols, width = features.shape
    tiles = lax.axis_size("sy") * lax.axis_size("sx")
    count = images * rows * cols * lax.axis_size("dp") * tiles
    inner_width = w_spatial.shape[3]
    current = features
    for block in range(BLOCKS):
        flat = current.reshape(-1, width)
        first = perturbed_product(
            flat, w_reduce[block], dir_reduce[0, block], dir_reduce[1, block], alpha_a, alpha_b
        )
        first = jax.nn.relu(
            normalize(first, gain_mid[block, 0], shift_mid[block, 0], count)
        ).astype(jnp.bfloat16)
        framed = padded_tile(first.reshape(images, rows, cols, inner_width))
        patches = jnp.concatenate(
            [framed[:, i : i + rows, j : j + cols, :] for i in range(3) for j in range(3)], axis=-1
        )
        patches = patches.reshape(-1, 9 * inner_width)
        spatial_base = w_spatial[block].reshape(9 * inner_width, -1)
        spatial_a = dir_spatial[0, block].reshape(9 * inner_width, -1)
        spatial_b = dir_spatial[1, block].reshape(9 * inner_width, -1)
        second = perturbed_product(patches, spatial_base, spatial_a, spatial_b, alpha_a, alpha_b)
        second = jax.nn.relu(
            normalize(second, gain_mid[block, 1], shift_mid[block, 1], count)
        ).astype(jnp.bfloat16)
        third = perturbed_product(
            second, w_expand[block], dir_expand[0, block], dir_expand[1, block], alpha_a, alpha_b
        )
        third = normalize(third, gain_out[block], shift_out[block], count)
        current = (
            jax.nn.relu(flat.astype(jnp.float32) + third)
            .astype(jnp.bfloat16)
            .reshape(images, rows, cols, width)
        )
    pooled_part = jnp.sum(current.astype(jnp.float32), axis=(1, 2))
    pooled = (lax.psum(pooled_part, ("sy", "sx")) / (rows * cols * tiles)).astype(jnp.bfloat16)
    class_a = dir_class[0]
    class_b = dir_class[1]
    norm_base, norm_a, norm_b = lax.psum(
        (
            jnp.sum(jnp.square(w_class.astype(jnp.float32)), axis=0),
            jnp.sum(jnp.square(class_a.astype(jnp.float32)), axis=0),
            jnp.sum(jnp.square(class_b.astype(jnp.float32)), axis=0),
        ),
        "dp",
    )
    ratio_a = jnp.sqrt(norm_base) / jnp.sqrt(norm_a + EPS_NORM)
    ratio_b = jnp.sqrt(norm_base) / jnp.sqrt(norm_b + EPS_NORM)
    local_class = (
        w_class.astype(jnp.float32)
        + alpha_a * ratio_a * class_a.astype(jnp.float32)
        + alpha_b * ratio_b * class_b.astype(jnp.float32)
    ).astype(jnp.bfloat16)
    logits = jnp.dot(
        pooled,
        lax.all_gather(local_class, "dp", axis=0, tiled=True),
        preferred_element_type=jnp.float32,
    )
    summed = jnp.log(jnp.sum(jnp.exp(logits), axis=1))
    classes = lax.broadcasted_iota(jnp.int32, logits.shape, 1)
    picked = jnp.sum(jnp.where(classes == labels[:, None], logits, 0.0), axis=1)
    image_loss = summed - picked
    mean_loss = lax.psum(jnp.sum(image_loss), "dp") / (images * lax.axis_size("dp"))
    return (current, image_loss, mean_loss)


F32 = jnp.float32
BF16 = jnp.bfloat16
NT = (((1,), (1,)), ((), ()))


def round_up(value, unit):
    return (value + unit - 1) // unit * unit


def rows_joined(blocks):
    count, rows, width = blocks.shape
    if rows % 16 == 0:
        return blocks.reshape(count * rows, width)
    return blocks.astype(F32).reshape(count * rows, width).astype(BF16)


def unit_ratio(base_sq, dir_sq):
    return jnp.sqrt(base_sq) / jnp.sqrt(dir_sq + EPS_NORM)


def section_kernel(
    parts,
    x_ref,
    labels_ref,
    grid_ref,
    wr_ref,
    ws_ref,
    we_ref,
    wc_ref,
    dr_ref,
    ds_ref,
    de_ref,
    dc_ref,
    gm_ref,
    sm_ref,
    go_ref,
    so_ref,
    out_ref,
    loss_ref,
    mean_ref,
    xs,
    edge,
    y2s,
    y3s,
    pr,
    ps,
    pe,
    pc,
    nc,
    tile_mid,
    tile_out,
    all_mid,
    all_out,
    halo_row,
    halo_col,
    halo_cor,
    pooled_parts,
    loss_parts,
    send,
    recv,
):
    rows, cols, width = x_ref.shape
    blocks = wr_ref.shape[0]
    mid = edge.shape[-1]
    pitch = edge.shape[1]
    flat = rows * pitch
    classes = wc_ref.shape[-1]
    last = pitch - 8
    me, my_y, my_x = lax.axis_index("dp"), lax.axis_index("sy"), lax.axis_index("sx")
    tile = my_y * 2 + my_x
    across = {"sy": 1 - my_y}
    beside = {"sx": 1 - my_x}
    corner = {"sy": 1 - my_y, "sx": 1 - my_x}
    quad = (beside, across, corner)

    def peer(d):
        return {"dp": lax.rem(me + d, parts)}

    def each_part(act):
        def step(d, carry):
            act(peer(d))
            return carry

        lax.fori_loop(1, parts, step, 0)

    counter = [0]

    def channel():
        counter[0] += 1
        return counter[0] - 1

    def push(source, target, link, device):
        pltpu.make_async_remote_copy(
            src_ref=source,
            dst_ref=target,
            send_sem=send.at[link],
            recv_sem=recv.at[link],
            device_id=device,
            device_id_type=pl.DeviceIdType.MESH,
        ).start()

    def arrived(view, link):
        pltpu.make_async_copy(view, view, recv.at[link]).wait()

    def left(view, link):
        pltpu.make_async_copy(view, view, send.at[link]).wait()

    pending = []

    def share_parts(buffer):
        link = channel()
        own = buffer.at[me]
        each_part(lambda device: push(own, own, link, device))
        view = buffer.at[pl.ds(0, parts - 1)]
        pending.append((view, link))
        return lambda: arrived(view, link)

    def share_tiles(buffer):
        link = channel()
        own = buffer.at[tile]
        for device in quad:
            push(own, own, link, device)
        view = buffer.at[pl.ds(0, 3)]
        pending.append((view, link))
        return lambda: arrived(view, link)

    barrier = pltpu.get_barrier_semaphore()

    def greet(device):
        pl.semaphore_signal(barrier, inc=1, device_id=device, device_id_type=pl.DeviceIdType.MESH)

    for device in quad:
        greet(device)
    each_part(greet)

    alpha = [(2.0 * grid_ref[k].astype(F32) + (1.0 - GRID)) * (1.0 / GRID) for k in range(2)]

    def square_sum(value):
        return jnp.sum(value * value, axis=-1, keepdims=True)

    for b in range(blocks):
        base, first, second = (v.astype(F32) for v in (wr_ref[b], dr_ref[0, b], dr_ref[1, b]))
        norm = square_sum(base)
        pr[me, b] = (
            base
            + alpha[0] * unit_ratio(norm, square_sum(first)) * first
            + alpha[1] * unit_ratio(norm, square_sum(second)) * second
        ).astype(BF16)
    pl.semaphore_wait(barrier, 3 + parts - 1)
    have_reduce = share_parts(pr)
    for b in range(blocks):
        base, first, second = (v.astype(F32) for v in (ws_ref[b], ds_ref[0, b], ds_ref[1, b]))
        norm, norm_a, norm_b = (
            jnp.sum(square_sum(v), axis=0) for v in (base, first, second)
        )
        value = (
            base
            + (alpha[0] * unit_ratio(norm, norm_a))[None] * first
            + (alpha[1] * unit_ratio(norm, norm_b))[None] * second
        )
        ps[me, b] = jnp.concatenate([value[t] for t in range(value.shape[0])], axis=-1).astype(BF16)
    have_spatial = share_parts(ps)
    for b in range(blocks):
        base, first, second = (v.astype(F32) for v in (we_ref[b], de_ref[0, b], de_ref[1, b]))
        norm = square_sum(base)
        pe[me, b] = (
            base
            + alpha[0] * unit_ratio(norm, square_sum(first)) * first
            + alpha[1] * unit_ratio(norm, square_sum(second)) * second
        ).astype(BF16)
    have_expand = share_parts(pe)
    class_arrays = [v.astype(F32) for v in (wc_ref[...], dc_ref[0], dc_ref[1])]
    nc[me] = jnp.concatenate(
        [jnp.sum(v * v, axis=0, keepdims=True) for v in class_arrays], axis=0
    )
    have_norms = share_parts(nc)

    xs[...] = jnp.zeros_like(xs)
    xs[:, 0:cols, :] = x_ref[...]

    inside = lax.broadcasted_iota(jnp.int32, (rows, pitch, 1), 1) < cols
    edge_row = lax.broadcasted_iota(jnp.int32, (rows + 2, pitch, 1), 0)
    edge_col = lax.broadcasted_iota(jnp.int32, (rows + 2, pitch, 1), 1)
    far_row = jnp.where(my_y == 0, rows + 1, 0)
    far_col = jnp.where(my_x == 0, cols, pitch - 1)
    valid = ((edge_row >= 1) & (edge_row <= rows) | (edge_row == far_row)) & (
        (edge_col < cols) | (edge_col == far_col)
    )
    near_row = jnp.where(my_y == 0, rows, 1)
    near_col = pl.multiple_of(jnp.where(my_x == 0, last, 0), 8)
    slot = far_col - last

    def local_stats(value):
        masked = jnp.where(inside, value, 0.0)
        mean = jnp.sum(masked, axis=(0, 1), keepdims=True)[0] / (rows * cols)
        centred = jnp.where(inside, value - mean[None], 0.0)
        return mean, jnp.sum(centred * centred, axis=(0, 1), keepdims=True)[0] / (rows * cols)

    def pooled_stats(buffer, r):
        means, spreads = buffer[r, :, 0:1, :], buffer[r, :, 1:2, :]
        mean = jnp.mean(means, axis=0)
        gap = means - mean[None]
        return mean, jnp.mean(spreads, axis=0) + jnp.mean(gap * gap, axis=0)

    def batch_stats(value, tiles, alls, r):
        mean, var = local_stats(value)
        tiles[r, tile, 0:1, :] = mean
        tiles[r, tile, 1:2, :] = var
        share_tiles(tiles.at[r])()
        mean, var = pooled_stats(tiles, r)
        alls[r, me, 0:1, :] = mean
        alls[r, me, 1:2, :] = var
        share_parts(alls.at[r])()
        mean, var = pooled_stats(alls, r)
        return mean, lax.rsqrt(var + EPS_BN)

    for b in range(blocks):
        if b == 0:
            have_reduce()
        w = rows_joined(pr[:, b])
        y = lax.dot_general(xs[...].reshape(flat, width), w, NT, preferred_element_type=F32)
        edge[1 : rows + 1] = y.reshape(rows, pitch, mid)
        links = (channel(), channel(), channel())
        push(edge.at[near_row], halo_row.at[b], links[0], across)
        push(
            edge.at[pl.ds(1, rows), pl.ds(near_col, 8), :], halo_col.at[b], links[1], beside
        )
        push(edge.at[near_row, pl.ds(near_col, 8), :], halo_cor.at[b], links[2], corner)
        mean, scale = batch_stats(edge[1 : rows + 1], tile_mid, all_mid, 2 * b)
        for view, link in zip((halo_row.at[b], halo_col.at[b], halo_cor.at[b]), links):
            left(view, link)
            arrived(view, link)
        shifted = pltpu.roll(halo_col[b].reshape(rows * 8, mid), 4, 0).reshape(rows, 8, mid)
        lane8 = lax.broadcasted_iota(jnp.int32, (rows, 8, 1), 1)
        edge[1 : rows + 1, last:pitch, :] = jnp.where(
            lane8 == slot, shifted, edge[1 : rows + 1, last:pitch, :]
        )
        edge[far_row] = halo_row[b]
        end8 = lax.broadcasted_iota(jnp.int32, (8, 1), 0)
        edge[far_row, last:pitch, :] = jnp.where(
            end8 == slot, pltpu.roll(halo_cor[b], 4, 0), halo_row[b, last:pitch, :]
        )
        gain = scale * gm_ref[b, 0:1]
        a = jnp.where(
            valid,
            jax.nn.relu((edge[...] - mean[None]) * gain[None] + sm_ref[b, 0:1][None]),
            0.0,
        )
        tall = (rows + 2) * pitch
        prev = pltpu.roll(a, 1, 1).reshape(tall, mid)
        after = pltpu.roll(a, pitch - 1, 1).reshape(tall, mid)
        wide = jnp.concatenate([prev, a.reshape(tall, mid), after], axis=-1).astype(BF16)
        if b == 0:
            have_norms()
            sums = jnp.sum(nc[...], axis=0)
            base_sq = sums[0:1]
            pc[me] = (
                class_arrays[0]
                + alpha[0] * unit_ratio(base_sq, sums[1:2]) * class_arrays[1]
                + alpha[1] * unit_ratio(base_sq, sums[2:3]) * class_arrays[2]
            ).astype(BF16)
            have_class = share_parts(pc)
            have_spatial()
        w = rows_joined(ps[:, b])
        span = 3 * mid
        y = sum(
            lax.dot_general(
                wide[i * pitch : i * pitch + flat],
                w[:, i * span : (i + 1) * span],
                NT,
                preferred_element_type=F32,
            )
            for i in range(3)
        )
        y2s[...] = y.reshape(rows, pitch, mid)
        mean, scale = batch_stats(y2s[...], tile_mid, all_mid, 2 * b + 1)
        gain = scale * gm_ref[b, 1:2]
        c = jax.nn.relu((y2s[...] - mean[None]) * gain[None] + sm_ref[b, 1:2][None])
        if b == 0:
            have_expand()
        w = rows_joined(pe[:, b])
        y = lax.dot_general(
            c.reshape(flat, mid).astype(BF16), w, NT, preferred_element_type=F32
        )
        y3s[...] = y.reshape(rows, pitch, width)
        mean, scale = batch_stats(y3s[...], tile_out, all_out, b)
        gain = scale * go_ref[b : b + 1]
        e = (y3s[...] - mean[None]) * gain[None] + so_ref[b : b + 1][None]
        xs[...] = jnp.where(inside, jax.nn.relu(xs[...].astype(F32) + e), 0.0).astype(BF16)

    final = xs[...]
    pooled_parts[tile] = jnp.sum(final.astype(F32), axis=(0, 1), keepdims=True)[0]
    have_pooled = share_tiles(pooled_parts)
    out_ref[...] = xs[:, 0:cols, :]
    have_class()
    have_pooled()
    total = jnp.sum(pooled_parts[...], axis=0)
    pooled = (total / (rows * cols * 4)).astype(BF16)
    logits = jnp.dot(pooled, rows_joined(pc[...]), preferred_element_type=F32)
    summed = jnp.log(jnp.sum(jnp.exp(logits), axis=1, keepdims=True))
    index = lax.broadcasted_iota(jnp.int32, logits.shape, 1)
    picked = jnp.sum(jnp.where(index == labels_ref[0], logits, 0.0), axis=1, keepdims=True)
    loss = jnp.broadcast_to(summed - picked, loss_ref.shape)
    loss_ref[...] = loss
    loss_parts[me] = loss
    share_parts(loss_parts)()
    mean_ref[...] = jnp.mean(loss_parts[...], axis=0)
    for view, link in pending:
        left(view, link)


def fused(mesh, *args):
    (features, labels, grid, w_reduce, w_spatial, w_expand, w_class) = args[:7]
    (dir_reduce, dir_spatial, dir_expand, dir_class) = args[7:11]
    parts = mesh.shape["dp"]
    _, rows, cols, width = features.shape
    blocks, mid = w_expand.shape[0], w_expand.shape[1]
    taps = w_spatial.shape[1] * w_spatial.shape[2]
    own_mid, own_out = w_reduce.shape[-1], w_expand.shape[-1]
    own_feat, classes = w_class.shape
    pitch = round_up(cols + 2, 8)

    def spatial(v, lead):
        return jnp.swapaxes(v, -1, -2).reshape(lead + (taps, own_mid, mid))

    operands = (
        features[0],
        labels,
        grid,
        jnp.swapaxes(w_reduce, -1, -2),
        spatial(w_spatial, (blocks,)),
        jnp.swapaxes(w_expand, -1, -2),
        w_class,
        jnp.swapaxes(dir_reduce, -1, -2),
        spatial(dir_spatial, (2, blocks)),
        jnp.swapaxes(dir_expand, -1, -2),
        dir_class,
    ) + tuple(args[11:])
    vmem = pl.BlockSpec(memory_space=pltpu.VMEM)
    smem = pl.BlockSpec(memory_space=pltpu.SMEM)
    links = 7 + 9 * blocks
    out, loss, mean_loss = pl.pallas_call(
        functools.partial(section_kernel, parts),
        out_shape=(
            jax.ShapeDtypeStruct((rows, cols, width), BF16),
            jax.ShapeDtypeStruct((1, 128), F32),
            jax.ShapeDtypeStruct((1, 128), F32),
        ),
        in_specs=[vmem, smem, smem] + [vmem] * 12,
        out_specs=(vmem, vmem, vmem),
        scratch_shapes=[
            pltpu.VMEM((rows, pitch, width), BF16),
            pltpu.VMEM((rows + 2, pitch, mid), F32),
            pltpu.VMEM((rows, pitch, mid), F32),
            pltpu.VMEM((rows, pitch, width), F32),
            pltpu.VMEM((parts, blocks, own_mid, width), BF16),
            pltpu.VMEM((parts, blocks, own_mid, taps * mid), BF16),
            pltpu.VMEM((parts, blocks, own_out, mid), BF16),
            pltpu.VMEM((parts, own_feat, classes), BF16),
            pltpu.VMEM((parts, 3, classes), F32),
            pltpu.VMEM((2 * blocks, 4, 2, mid), F32),
            pltpu.VMEM((blocks, 4, 2, width), F32),
            pltpu.VMEM((2 * blocks, parts, 2, mid), F32),
            pltpu.VMEM((blocks, parts, 2, width), F32),
            pltpu.VMEM((blocks, pitch, mid), F32),
            pltpu.VMEM((blocks, rows, 8, mid), F32),
            pltpu.VMEM((blocks, 8, mid), F32),
            pltpu.VMEM((4, 1, width), F32),
            pltpu.VMEM((parts, 1, 128), F32),
            pltpu.SemaphoreType.DMA((links,)),
            pltpu.SemaphoreType.DMA((links,)),
        ],
        compiler_params=pltpu.CompilerParams(
            collective_id=0, has_side_effects=True, vmem_limit_bytes=56 * 2**20
        ),
    )(*operands)
    return out[None], loss[0, 0:1], mean_loss[0, 0]


def body(mesh, *args):
    features = args[0]
    plain = mesh.shape["sy"] == 2 and mesh.shape["sx"] == 2 and mesh.shape["dp"] > 1
    if plain and features.shape[0] == 1 and features.shape[2] % 8 == 4:
        return fused(mesh, *args)
    return per_device(*args)


def solution(mesh):
    in_specs = (
        P("dp", "sy", "sx", None),
        P("dp"),
        P(),
        P(None, None, "dp"),
        P(None, None, None, None, "dp"),
        P(None, None, "dp"),
        P("dp", None),
        P(None, None, None, "dp"),
        P(None, None, None, None, None, "dp"),
        P(None, None, None, "dp"),
        P(None, "dp", None),
        P(),
        P(),
        P(),
        P(),
    )
    out_specs = (P("dp", "sy", "sx", None), P("dp"), P())
    return jax.shard_map(
        functools.partial(body, mesh), mesh=mesh, in_specs=in_specs, out_specs=out_specs, check_vma=False
    )
```

```python
import functools

import jax
import jax.numpy as jnp
from jax import lax
from jax.experimental import pallas as pl
from jax.experimental.pallas import tpu as pltpu
from jax.sharding import PartitionSpec as P

BLOCKS = 3
GRID = 50


EPS_NORM = 1e-06
EPS_BN = 1e-05


def extended(cells, sides, width):
    for axis, dim in sides:
        count = lax.axis_size(axis)
        ends = count - 1
        head = lax.slice_in_dim(cells, 0, width, axis=dim)
        tail = lax.slice_in_dim(cells, cells.shape[dim] - width, cells.shape[dim], axis=dim)
        cells = jnp.concatenate(
            [
                lax.ppermute(tail, axis, [(i, (i + 1) % count) for i in range(ends)]),
                cells,
                lax.ppermute(head, axis, [((i + 1) % count, i) for i in range(ends)]),
            ],
            axis=dim,
        )
    return cells


def coefficients(grid):
    values = grid.astype(jnp.float32)
    alpha = (2.0 * values + 1.0 - GRID) / GRID
    return (alpha[0], alpha[1])


def filter_ratio(base, direction):
    base_norm = jnp.sqrt(jnp.sum(jnp.square(base.astype(jnp.float32)), axis=0, keepdims=True))
    dir_norm = jnp.sqrt(
        jnp.sum(jnp.square(direction.astype(jnp.float32)), axis=0, keepdims=True) + EPS_NORM
    )
    return base_norm / dir_norm


def combine_filters(base, dir_a, dir_b, alpha_a, alpha_b):
    ratio_a = filter_ratio(base, dir_a)
    ratio_b = filter_ratio(base, dir_b)
    value = (
        base.astype(jnp.float32)
        + alpha_a * ratio_a * dir_a.astype(jnp.float32)
        + alpha_b * ratio_b * dir_b.astype(jnp.float32)
    )
    return value.astype(jnp.bfloat16)


def perturbed_product(left, base, dir_a, dir_b, alpha_a, alpha_b):
    local = combine_filters(base, dir_a, dir_b, alpha_a, alpha_b)
    return jnp.dot(
        left, lax.all_gather(local, "dp", axis=1, tiled=True), preferred_element_type=jnp.float32
    )


def normalize(y, gain, shift, count):
    mean = lax.psum(jnp.sum(y, axis=0), ("dp", "sy", "sx")) / count
    centred = y - mean
    var = lax.psum(jnp.sum(centred * centred, axis=0), ("dp", "sy", "sx")) / count
    return centred * lax.rsqrt(var + EPS_BN) * gain + shift


def padded_tile(inner):
    return extended(inner, (("sy", 1), ("sx", 2)), 1)


def per_device(
    features,
    labels,
    grid,
    w_reduce,
    w_spatial,
    w_expand,
    w_class,
    dir_reduce,
    dir_spatial,
    dir_expand,
    dir_class,
    gain_mid,
    shift_mid,
    gain_out,
    shift_out,
):
    alpha_a, alpha_b = coefficients(grid)
    images, rows, cols, width = features.shape
    tiles = lax.axis_size("sy") * lax.axis_size("sx")
    count = images * rows * cols * lax.axis_size("dp") * tiles
    inner_width = w_spatial.shape[3]
    current = features
    for block in range(BLOCKS):
        flat = current.reshape(-1, width)
        first = perturbed_product(
            flat, w_reduce[block], dir_reduce[0, block], dir_reduce[1, block], alpha_a, alpha_b
        )
        first = jax.nn.relu(
            normalize(first, gain_mid[block, 0], shift_mid[block, 0], count)
        ).astype(jnp.bfloat16)
        framed = padded_tile(first.reshape(images, rows, cols, inner_width))
        patches = jnp.concatenate(
            [framed[:, i : i + rows, j : j + cols, :] for i in range(3) for j in range(3)], axis=-1
        )
        patches = patches.reshape(-1, 9 * inner_width)
        spatial_base = w_spatial[block].reshape(9 * inner_width, -1)
        spatial_a = dir_spatial[0, block].reshape(9 * inner_width, -1)
        spatial_b = dir_spatial[1, block].reshape(9 * inner_width, -1)
        second = perturbed_product(patches, spatial_base, spatial_a, spatial_b, alpha_a, alpha_b)
        second = jax.nn.relu(
            normalize(second, gain_mid[block, 1], shift_mid[block, 1], count)
        ).astype(jnp.bfloat16)
        third = perturbed_product(
            second, w_expand[block], dir_expand[0, block], dir_expand[1, block], alpha_a, alpha_b
        )
        third = normalize(third, gain_out[block], shift_out[block], count)
        current = (
            jax.nn.relu(flat.astype(jnp.float32) + third)
            .astype(jnp.bfloat16)
            .reshape(images, rows, cols, width)
        )
    pooled_part = jnp.sum(current.astype(jnp.float32), axis=(1, 2))
    pooled = (lax.psum(pooled_part, ("sy", "sx")) / (rows * cols * tiles)).astype(jnp.bfloat16)
    class_a = dir_class[0]
    class_b = dir_class[1]
    norm_base, norm_a, norm_b = lax.psum(
        (
            jnp.sum(jnp.square(w_class.astype(jnp.float32)), axis=0),
            jnp.sum(jnp.square(class_a.astype(jnp.float32)), axis=0),
            jnp.sum(jnp.square(class_b.astype(jnp.float32)), axis=0),
        ),
        "dp",
    )
    ratio_a = jnp.sqrt(norm_base) / jnp.sqrt(norm_a + EPS_NORM)
    ratio_b = jnp.sqrt(norm_base) / jnp.sqrt(norm_b + EPS_NORM)
    local_class = (
        w_class.astype(jnp.float32)
        + alpha_a * ratio_a * class_a.astype(jnp.float32)
        + alpha_b * ratio_b * class_b.astype(jnp.float32)
    ).astype(jnp.bfloat16)
    logits = jnp.dot(
        pooled,
        lax.all_gather(local_class, "dp", axis=0, tiled=True),
        preferred_element_type=jnp.float32,
    )
    summed = jnp.log(jnp.sum(jnp.exp(logits), axis=1))
    classes = lax.broadcasted_iota(jnp.int32, logits.shape, 1)
    picked = jnp.sum(jnp.where(classes == labels[:, None], logits, 0.0), axis=1)
    image_loss = summed - picked
    mean_loss = lax.psum(jnp.sum(image_loss), "dp") / (images * lax.axis_size("dp"))
    return (current, image_loss, mean_loss)


F32 = jnp.float32
BF16 = jnp.bfloat16
NT = (((1,), (1,)), ((), ()))


def round_up(value, unit):
    return (value + unit - 1) // unit * unit


def rows_joined(blocks):
    count, rows, width = blocks.shape
    if rows % 16 == 0:
        return blocks.reshape(count * rows, width)
    return blocks.astype(F32).reshape(count * rows, width).astype(BF16)


def unit_ratio(base_sq, dir_sq):
    return jnp.sqrt(base_sq) / jnp.sqrt(dir_sq + EPS_NORM)


def section_kernel(
    parts,
    x_ref,
    labels_ref,
    grid_ref,
    wr_ref,
    ws_ref,
    we_ref,
    wc_ref,
    dr_ref,
    ds_ref,
    de_ref,
    dc_ref,
    gm_ref,
    sm_ref,
    go_ref,
    so_ref,
    out_ref,
    loss_ref,
    mean_ref,
    xs,
    edge,
    y2s,
    y3s,
    pr,
    ps,
    pe,
    pc,
    nc,
    all_mid,
    all_out,
    halo_row,
    halo_col,
    halo_cor,
    pooled_parts,
    send,
    recv,
):
    rows, cols, width = x_ref.shape
    blocks = wr_ref.shape[0]
    mid = edge.shape[-1]
    pitch = edge.shape[1]
    flat = rows * pitch
    classes = wc_ref.shape[-1]
    last = pitch - 8
    me, my_y, my_x = lax.axis_index("dp"), lax.axis_index("sy"), lax.axis_index("sx")
    tiles = 4
    devices = parts * tiles
    place = (me * 2 + my_y) * 2 + my_x
    across = {"sy": 1 - my_y}
    beside = {"sx": 1 - my_x}
    corner = {"sy": 1 - my_y, "sx": 1 - my_x}

    def peer(d):
        return {"dp": lax.rem(me + d, parts)}

    def each_part(act):
        def step(d, carry):
            act(peer(d))
            return carry

        lax.fori_loop(1, parts, step, 0)

    counter = [0]

    def channel():
        counter[0] += 1
        return counter[0] - 1

    def push(source, target, link, device):
        pltpu.make_async_remote_copy(
            src_ref=source,
            dst_ref=target,
            send_sem=send.at[link],
            recv_sem=recv.at[link],
            device_id=device,
            device_id_type=pl.DeviceIdType.MESH,
        ).start()

    def arrived(view, link):
        pltpu.make_async_copy(view, view, recv.at[link]).wait()

    def left(view, link):
        pltpu.make_async_copy(view, view, send.at[link]).wait()

    pending = []

    def share_parts(buffer):
        link = channel()
        own = buffer.at[me]
        each_part(lambda device: push(own, own, link, device))
        view = buffer.at[pl.ds(0, parts - 1)]
        pending.append((view, link))
        return lambda: arrived(view, link)

    def share_all(buffer):
        link = channel()
        own = buffer.at[place]

        def step(d, carry):
            other = lax.rem(place + d, devices)
            device = {
                "dp": lax.div(other, tiles),
                "sy": lax.rem(lax.div(other, 2), 2),
                "sx": lax.rem(other, 2),
            }
            push(own, own, link, device)
            return carry

        lax.fori_loop(1, devices, step, 0)
        view = buffer.at[pl.ds(0, devices - 1)]
        pending.append((view, link))
        return lambda: arrived(view, link)

    barrier = pltpu.get_barrier_semaphore()

    def greet(device):
        pl.semaphore_signal(barrier, inc=1, device_id=device, device_id_type=pl.DeviceIdType.MESH)

    def greet_step(d, carry):
        other = lax.rem(place + d, devices)
        greet(
            {
                "dp": lax.div(other, tiles),
                "sy": lax.rem(lax.div(other, 2), 2),
                "sx": lax.rem(other, 2),
            }
        )
        return carry

    lax.fori_loop(1, devices, greet_step, 0)

    alpha = [(2.0 * grid_ref[k].astype(F32) + (1.0 - GRID)) * (1.0 / GRID) for k in range(2)]

    def square_sum(value):
        return jnp.sum(value * value, axis=-1, keepdims=True)

    def pointwise_filters(base_ref, dir_ref, target, b):
        base, first, second = (v.astype(F32) for v in (base_ref[b], dir_ref[0, b], dir_ref[1, b]))
        norm = square_sum(base)
        target[b, me] = (
            base
            + alpha[0] * unit_ratio(norm, square_sum(first)) * first
            + alpha[1] * unit_ratio(norm, square_sum(second)) * second
        ).astype(BF16)

    def send_reduce(b):
        have[("r", b)] = share_parts(pr.at[b])

    def send_spatial(b):
        base, first, second = (v.astype(F32) for v in (ws_ref[b], ds_ref[0, b], ds_ref[1, b]))
        norm, norm_a, norm_b = (
            jnp.sum(square_sum(v), axis=0) for v in (base, first, second)
        )
        value = (
            base
            + (alpha[0] * unit_ratio(norm, norm_a))[None] * first
            + (alpha[1] * unit_ratio(norm, norm_b))[None] * second
        )
        ps[b, me] = jnp.concatenate([value[t] for t in range(value.shape[0])], axis=-1).astype(BF16)
        have[("s", b)] = share_parts(ps.at[b])

    def send_expand(b):
        pointwise_filters(we_ref, de_ref, pe, b)
        have[("e", b)] = share_parts(pe.at[b])

    def class_arrays():
        return [v.astype(F32) for v in (wc_ref[...], dc_ref[0], dc_ref[1])]

    def send_norms():
        nc[me] = jnp.concatenate(
            [jnp.sum(v * v, axis=0, keepdims=True) for v in class_arrays()], axis=0
        )
        have["norms"] = share_parts(nc)

    def send_class():
        have["norms"]()
        sums = jnp.sum(nc[...], axis=0)
        base_sq = sums[0:1]
        base, first, second = class_arrays()
        pc[me] = (
            base
            + alpha[0] * unit_ratio(base_sq, sums[1:2]) * first
            + alpha[1] * unit_ratio(base_sq, sums[2:3]) * second
        ).astype(BF16)
        have["class"] = share_parts(pc)

    def ready(kind, source, b):
        have[(kind, b)]()
        return rows_joined(source[b])

    have = {}
    pointwise_filters(wr_ref, dr_ref, pr, 0)
    pl.semaphore_wait(barrier, devices - 1)
    send_reduce(0)
    send_spatial(0)
    send_expand(0)

    xs[...] = jnp.zeros_like(xs)
    xs[:, 0:cols, :] = x_ref[...]

    inside = lax.broadcasted_iota(jnp.int32, (rows, pitch, 1), 1) < cols
    edge_row = lax.broadcasted_iota(jnp.int32, (rows + 2, pitch, 1), 0)
    edge_col = lax.broadcasted_iota(jnp.int32, (rows + 2, pitch, 1), 1)
    far_row = jnp.where(my_y == 0, rows + 1, 0)
    far_col = jnp.where(my_x == 0, cols, pitch - 1)
    valid = ((edge_row >= 1) & (edge_row <= rows) | (edge_row == far_row)) & (
        (edge_col < cols) | (edge_col == far_col)
    )
    near_row = jnp.where(my_y == 0, rows, 1)
    near_col = pl.multiple_of(jnp.where(my_x == 0, last, 0), 8)
    slot = far_col - last

    def local_stats(value):
        masked = jnp.where(inside, value, 0.0)
        mean = jnp.sum(masked, axis=(0, 1), keepdims=True)[0] / (rows * cols)
        centred = jnp.where(inside, value - mean[None], 0.0)
        return mean, jnp.sum(centred * centred, axis=(0, 1), keepdims=True)[0] / (rows * cols)

    def pooled_stats(buffer, r):
        means, spreads = buffer[r, :, 0:1, :], buffer[r, :, 1:2, :]
        mean = jnp.mean(means, axis=0)
        gap = means - mean[None]
        return mean, jnp.mean(spreads, axis=0) + jnp.mean(gap * gap, axis=0)

    def batch_stats(value, alls, r, meanwhile):
        mean, var = local_stats(value)
        alls[r, place, 0:1, :] = mean
        alls[r, place, 1:2, :] = var
        come = share_all(alls.at[r])
        other = meanwhile()
        come()
        mean, var = pooled_stats(alls, r)
        return mean, lax.rsqrt(var + EPS_BN), other

    def after_first(b):
        if b == 0:
            send_norms()
        elif b == 1 and blocks > 1:
            send_class()
        return ready("s", ps, b)

    def after_second(b):
        if b + 1 < blocks:
            pointwise_filters(wr_ref, dr_ref, pr, b + 1)
            send_reduce(b + 1)
            send_spatial(b + 1)
        return ready("e", pe, b)

    def after_third(b):
        if b + 1 < blocks:
            send_expand(b + 1)
            return ready("r", pr, b + 1)
        if "class" not in have:
            send_class()
        return None

    w_reduce = ready("r", pr, 0)
    for b in range(blocks):
        y = lax.dot_general(
            xs[...].reshape(flat, width), w_reduce, NT, preferred_element_type=F32
        )
        edge[1 : rows + 1] = y.reshape(rows, pitch, mid)
        links = (channel(), channel(), channel())
        push(edge.at[near_row], halo_row.at[b], links[0], across)
        push(
            edge.at[pl.ds(1, rows), pl.ds(near_col, 8), :], halo_col.at[b], links[1], beside
        )
        push(edge.at[near_row, pl.ds(near_col, 8), :], halo_cor.at[b], links[2], corner)
        mean, scale, w = batch_stats(
            edge[1 : rows + 1], all_mid, 2 * b, functools.partial(after_first, b)
        )
        for view, link in zip((halo_row.at[b], halo_col.at[b], halo_cor.at[b]), links):
            left(view, link)
            arrived(view, link)
        shifted = pltpu.roll(halo_col[b].reshape(rows * 8, mid), 4, 0).reshape(rows, 8, mid)
        lane8 = lax.broadcasted_iota(jnp.int32, (rows, 8, 1), 1)
        edge[1 : rows + 1, last:pitch, :] = jnp.where(
            lane8 == slot, shifted, edge[1 : rows + 1, last:pitch, :]
        )
        edge[far_row] = halo_row[b]
        end8 = lax.broadcasted_iota(jnp.int32, (8, 1), 0)
        edge[far_row, last:pitch, :] = jnp.where(
            end8 == slot, pltpu.roll(halo_cor[b], 4, 0), halo_row[b, last:pitch, :]
        )
        gain = scale * gm_ref[b, 0:1]
        a = jnp.where(
            valid,
            jax.nn.relu((edge[...] - mean[None]) * gain[None] + sm_ref[b, 0:1][None]),
            0.0,
        )
        tall = (rows + 2) * pitch
        prev = pltpu.roll(a, 1, 1).reshape(tall, mid)
        after = pltpu.roll(a, pitch - 1, 1).reshape(tall, mid)
        wide = jnp.concatenate([prev, a.reshape(tall, mid), after], axis=-1).astype(BF16)
        span = 3 * mid
        y = sum(
            lax.dot_general(
                wide[i * pitch : i * pitch + flat],
                w[:, i * span : (i + 1) * span],
                NT,
                preferred_element_type=F32,
            )
            for i in range(3)
        )
        y2s[...] = y.reshape(rows, pitch, mid)
        mean, scale, w = batch_stats(
            y2s[...], all_mid, 2 * b + 1, functools.partial(after_second, b)
        )
        gain = scale * gm_ref[b, 1:2]
        c = jax.nn.relu((y2s[...] - mean[None]) * gain[None] + sm_ref[b, 1:2][None])
        y = lax.dot_general(
            c.reshape(flat, mid).astype(BF16), w, NT, preferred_element_type=F32
        )
        y3s[...] = y.reshape(rows, pitch, width)
        mean, scale, w_reduce = batch_stats(
            y3s[...], all_out, b, functools.partial(after_third, b)
        )
        gain = scale * go_ref[b : b + 1]
        e = (y3s[...] - mean[None]) * gain[None] + so_ref[b : b + 1][None]
        xs[...] = jnp.where(inside, jax.nn.relu(xs[...].astype(F32) + e), 0.0).astype(BF16)

    final = xs[...]
    pooled_parts[place, 0:1, :] = jnp.sum(final.astype(F32), axis=(0, 1), keepdims=True)[0]
    pooled_parts[place, 1:2, :] = jnp.full((1, width), labels_ref[0].astype(F32))
    have_pooled = share_all(pooled_parts)
    out_ref[...] = xs[:, 0:cols, :]
    have["class"]()
    w = rows_joined(pc[...])
    have_pooled()
    by_image = [
        functools.reduce(jnp.add, [pooled_parts[i * tiles + t, 0:1, :] for t in range(tiles)])
        for i in range(parts)
    ]
    pooled = (jnp.concatenate(by_image, axis=0) / (rows * cols * tiles)).astype(BF16)
    wanted = jnp.concatenate([pooled_parts[i * tiles, 1:2, 0:1] for i in range(parts)], axis=0)
    logits = jnp.dot(pooled, w, preferred_element_type=F32)
    summed = jnp.log(jnp.sum(jnp.exp(logits), axis=1, keepdims=True))
    index = lax.broadcasted_iota(jnp.int32, logits.shape, 1).astype(F32)
    picked = jnp.sum(jnp.where(index == wanted, logits, 0.0), axis=1, keepdims=True)
    losses = summed - picked
    image = lax.broadcasted_iota(jnp.int32, losses.shape, 0)
    loss_ref[...] = jnp.broadcast_to(
        jnp.sum(jnp.where(image == me, losses, 0.0), axis=0, keepdims=True), loss_ref.shape
    )
    mean_ref[...] = jnp.broadcast_to(
        jnp.sum(losses, axis=0, keepdims=True) / parts, mean_ref.shape
    )
    for view, link in pending:
        left(view, link)


def fused(mesh, *args):
    (features, labels, grid, w_reduce, w_spatial, w_expand, w_class) = args[:7]
    (dir_reduce, dir_spatial, dir_expand, dir_class) = args[7:11]
    parts = mesh.shape["dp"]
    _, rows, cols, width = features.shape
    blocks, mid = w_expand.shape[0], w_expand.shape[1]
    taps = w_spatial.shape[1] * w_spatial.shape[2]
    own_mid, own_out = w_reduce.shape[-1], w_expand.shape[-1]
    own_feat, classes = w_class.shape
    pitch = round_up(cols + 2, 8)

    def spatial(v, lead):
        return jnp.swapaxes(v, -1, -2).reshape(lead + (taps, own_mid, mid))

    operands = (
        features[0],
        labels,
        grid,
        jnp.swapaxes(w_reduce, -1, -2),
        spatial(w_spatial, (blocks,)),
        jnp.swapaxes(w_expand, -1, -2),
        w_class,
        jnp.swapaxes(dir_reduce, -1, -2),
        spatial(dir_spatial, (2, blocks)),
        jnp.swapaxes(dir_expand, -1, -2),
        dir_class,
    ) + tuple(args[11:])
    vmem = pl.BlockSpec(memory_space=pltpu.VMEM)
    smem = pl.BlockSpec(memory_space=pltpu.SMEM)
    links = 3 + 9 * blocks
    out, loss, mean_loss = pl.pallas_call(
        functools.partial(section_kernel, parts),
        out_shape=(
            jax.ShapeDtypeStruct((rows, cols, width), BF16),
            jax.ShapeDtypeStruct((1, 128), F32),
            jax.ShapeDtypeStruct((1, 128), F32),
        ),
        in_specs=[vmem, smem, smem] + [vmem] * 12,
        out_specs=(vmem, vmem, vmem),
        scratch_shapes=[
            pltpu.VMEM((rows, pitch, width), BF16),
            pltpu.VMEM((rows + 2, pitch, mid), F32),
            pltpu.VMEM((rows, pitch, mid), F32),
            pltpu.VMEM((rows, pitch, width), F32),
            pltpu.VMEM((blocks, parts, own_mid, width), BF16),
            pltpu.VMEM((blocks, parts, own_mid, taps * mid), BF16),
            pltpu.VMEM((blocks, parts, own_out, mid), BF16),
            pltpu.VMEM((parts, own_feat, classes), BF16),
            pltpu.VMEM((parts, 3, classes), F32),
            pltpu.VMEM((2 * blocks, parts * 4, 2, mid), F32),
            pltpu.VMEM((blocks, parts * 4, 2, width), F32),
            pltpu.VMEM((blocks, pitch, mid), F32),
            pltpu.VMEM((blocks, rows, 8, mid), F32),
            pltpu.VMEM((blocks, 8, mid), F32),
            pltpu.VMEM((parts * 4, 2, width), F32),
            pltpu.SemaphoreType.DMA((links,)),
            pltpu.SemaphoreType.DMA((links,)),
        ],
        compiler_params=pltpu.CompilerParams(
            collective_id=0, has_side_effects=True, vmem_limit_bytes=56 * 2**20
        ),
    )(*operands)
    return out[None], loss[0, 0:1], mean_loss[0, 0]


def body(mesh, *args):
    features = args[0]
    plain = mesh.shape["sy"] == 2 and mesh.shape["sx"] == 2 and mesh.shape["dp"] > 1
    if plain and features.shape[0] == 1 and features.shape[2] % 8 == 4:
        return fused(mesh, *args)
    return per_device(*args)


def solution(mesh):
    in_specs = (
        P("dp", "sy", "sx", None),
        P("dp"),
        P(),
        P(None, None, "dp"),
        P(None, None, None, None, "dp"),
        P(None, None, "dp"),
        P("dp", None),
        P(None, None, None, "dp"),
        P(None, None, None, None, None, "dp"),
        P(None, None, None, "dp"),
        P(None, "dp", None),
        P(),
        P(),
        P(),
        P(),
    )
    out_specs = (P("dp", "sy", "sx", None), P("dp"), P())
    return jax.shard_map(
        functools.partial(body, mesh), mesh=mesh, in_specs=in_specs, out_specs=out_specs, check_vma=False
    )
```

```python
import functools

import jax
import jax.numpy as jnp
from jax import lax
from jax.experimental import pallas as pl
from jax.experimental.pallas import tpu as pltpu
from jax.sharding import PartitionSpec as P

BLOCKS = 3
GRID = 50


EPS_NORM = 1e-06
EPS_BN = 1e-05


def extended(cells, sides, width):
    for axis, dim in sides:
        count = lax.axis_size(axis)
        ends = count - 1
        head = lax.slice_in_dim(cells, 0, width, axis=dim)
        tail = lax.slice_in_dim(cells, cells.shape[dim] - width, cells.shape[dim], axis=dim)
        cells = jnp.concatenate(
            [
                lax.ppermute(tail, axis, [(i, (i + 1) % count) for i in range(ends)]),
                cells,
                lax.ppermute(head, axis, [((i + 1) % count, i) for i in range(ends)]),
            ],
            axis=dim,
        )
    return cells


def coefficients(grid):
    values = grid.astype(jnp.float32)
    alpha = (2.0 * values + 1.0 - GRID) / GRID
    return (alpha[0], alpha[1])


def filter_ratio(base, direction):
    base_norm = jnp.sqrt(jnp.sum(jnp.square(base.astype(jnp.float32)), axis=0, keepdims=True))
    dir_norm = jnp.sqrt(
        jnp.sum(jnp.square(direction.astype(jnp.float32)), axis=0, keepdims=True) + EPS_NORM
    )
    return base_norm / dir_norm


def combine_filters(base, dir_a, dir_b, alpha_a, alpha_b):
    ratio_a = filter_ratio(base, dir_a)
    ratio_b = filter_ratio(base, dir_b)
    value = (
        base.astype(jnp.float32)
        + alpha_a * ratio_a * dir_a.astype(jnp.float32)
        + alpha_b * ratio_b * dir_b.astype(jnp.float32)
    )
    return value.astype(jnp.bfloat16)


def perturbed_product(left, base, dir_a, dir_b, alpha_a, alpha_b):
    local = combine_filters(base, dir_a, dir_b, alpha_a, alpha_b)
    return jnp.dot(
        left, lax.all_gather(local, "dp", axis=1, tiled=True), preferred_element_type=jnp.float32
    )


def normalize(y, gain, shift, count):
    mean = lax.psum(jnp.sum(y, axis=0), ("dp", "sy", "sx")) / count
    centred = y - mean
    var = lax.psum(jnp.sum(centred * centred, axis=0), ("dp", "sy", "sx")) / count
    return centred * lax.rsqrt(var + EPS_BN) * gain + shift


def padded_tile(inner):
    return extended(inner, (("sy", 1), ("sx", 2)), 1)


def per_device(
    features,
    labels,
    grid,
    w_reduce,
    w_spatial,
    w_expand,
    w_class,
    dir_reduce,
    dir_spatial,
    dir_expand,
    dir_class,
    gain_mid,
    shift_mid,
    gain_out,
    shift_out,
):
    alpha_a, alpha_b = coefficients(grid)
    images, rows, cols, width = features.shape
    tiles = lax.axis_size("sy") * lax.axis_size("sx")
    count = images * rows * cols * lax.axis_size("dp") * tiles
    inner_width = w_spatial.shape[3]
    current = features
    for block in range(BLOCKS):
        flat = current.reshape(-1, width)
        first = perturbed_product(
            flat, w_reduce[block], dir_reduce[0, block], dir_reduce[1, block], alpha_a, alpha_b
        )
        first = jax.nn.relu(
            normalize(first, gain_mid[block, 0], shift_mid[block, 0], count)
        ).astype(jnp.bfloat16)
        framed = padded_tile(first.reshape(images, rows, cols, inner_width))
        patches = jnp.concatenate(
            [framed[:, i : i + rows, j : j + cols, :] for i in range(3) for j in range(3)], axis=-1
        )
        patches = patches.reshape(-1, 9 * inner_width)
        spatial_base = w_spatial[block].reshape(9 * inner_width, -1)
        spatial_a = dir_spatial[0, block].reshape(9 * inner_width, -1)
        spatial_b = dir_spatial[1, block].reshape(9 * inner_width, -1)
        second = perturbed_product(patches, spatial_base, spatial_a, spatial_b, alpha_a, alpha_b)
        second = jax.nn.relu(
            normalize(second, gain_mid[block, 1], shift_mid[block, 1], count)
        ).astype(jnp.bfloat16)
        third = perturbed_product(
            second, w_expand[block], dir_expand[0, block], dir_expand[1, block], alpha_a, alpha_b
        )
        third = normalize(third, gain_out[block], shift_out[block], count)
        current = (
            jax.nn.relu(flat.astype(jnp.float32) + third)
            .astype(jnp.bfloat16)
            .reshape(images, rows, cols, width)
        )
    pooled_part = jnp.sum(current.astype(jnp.float32), axis=(1, 2))
    pooled = (lax.psum(pooled_part, ("sy", "sx")) / (rows * cols * tiles)).astype(jnp.bfloat16)
    class_a = dir_class[0]
    class_b = dir_class[1]
    norm_base, norm_a, norm_b = lax.psum(
        (
            jnp.sum(jnp.square(w_class.astype(jnp.float32)), axis=0),
            jnp.sum(jnp.square(class_a.astype(jnp.float32)), axis=0),
            jnp.sum(jnp.square(class_b.astype(jnp.float32)), axis=0),
        ),
        "dp",
    )
    ratio_a = jnp.sqrt(norm_base) / jnp.sqrt(norm_a + EPS_NORM)
    ratio_b = jnp.sqrt(norm_base) / jnp.sqrt(norm_b + EPS_NORM)
    local_class = (
        w_class.astype(jnp.float32)
        + alpha_a * ratio_a * class_a.astype(jnp.float32)
        + alpha_b * ratio_b * class_b.astype(jnp.float32)
    ).astype(jnp.bfloat16)
    logits = jnp.dot(
        pooled,
        lax.all_gather(local_class, "dp", axis=0, tiled=True),
        preferred_element_type=jnp.float32,
    )
    summed = jnp.log(jnp.sum(jnp.exp(logits), axis=1))
    classes = lax.broadcasted_iota(jnp.int32, logits.shape, 1)
    picked = jnp.sum(jnp.where(classes == labels[:, None], logits, 0.0), axis=1)
    image_loss = summed - picked
    mean_loss = lax.psum(jnp.sum(image_loss), "dp") / (images * lax.axis_size("dp"))
    return (current, image_loss, mean_loss)


F32 = jnp.float32
BF16 = jnp.bfloat16
NT = (((1,), (1,)), ((), ()))


def round_up(value, unit):
    return (value + unit - 1) // unit * unit


def rows_joined(blocks):
    count, rows, width = blocks.shape
    if rows % 16 == 0:
        return blocks.reshape(count * rows, width)
    return blocks.astype(F32).reshape(count * rows, width).astype(BF16)


def unit_ratio(base_sq, dir_sq):
    return jnp.sqrt(base_sq) / jnp.sqrt(dir_sq + EPS_NORM)


def section_kernel(
    parts,
    x_ref,
    labels_ref,
    grid_ref,
    wr_ref,
    ws_ref,
    we_ref,
    wc_ref,
    dr_ref,
    ds_ref,
    de_ref,
    dc_ref,
    gm_ref,
    sm_ref,
    go_ref,
    so_ref,
    out_ref,
    loss_ref,
    mean_ref,
    xs,
    edge,
    y2s,
    y3s,
    pr,
    ps,
    pe,
    pc,
    nc,
    all_mid,
    all_out,
    halo_row,
    halo_col,
    halo_cor,
    pooled_parts,
    send,
    recv,
):
    rows, cols, width = x_ref.shape
    blocks = wr_ref.shape[0]
    mid = edge.shape[-1]
    pitch = edge.shape[1]
    flat = rows * pitch
    classes = wc_ref.shape[-1]
    last = pitch - 8
    me, my_y, my_x = lax.axis_index("dp"), lax.axis_index("sy"), lax.axis_index("sx")
    tiles = 4
    devices = parts * tiles
    place = (me * 2 + my_y) * 2 + my_x
    across = {"sy": 1 - my_y}
    beside = {"sx": 1 - my_x}
    corner = {"sy": 1 - my_y, "sx": 1 - my_x}

    sides_y, sides_x = (my_y, 1 - my_y), (my_x, 1 - my_x)

    def peer(d):
        other = me + d
        return {"dp": jnp.where(other >= parts, other - parts, other)}

    def each_device(act):
        for k in range(1, tiles):
            act({"sy": sides_y[k // 2], "sx": sides_x[k % 2]})

        def step(d, carry):
            for k in range(tiles):
                act({**peer(d), "sy": sides_y[k // 2], "sx": sides_x[k % 2]})
            return carry

        lax.fori_loop(1, parts, step, 0)

    def each_part(act):
        def step(d, carry):
            act(peer(d))
            return carry

        lax.fori_loop(1, parts, step, 0)

    counter = [0]

    def channel():
        counter[0] += 1
        return counter[0] - 1

    def push(source, target, link, device):
        pltpu.make_async_remote_copy(
            src_ref=source,
            dst_ref=target,
            send_sem=send.at[link],
            recv_sem=recv.at[link],
            device_id=device,
            device_id_type=pl.DeviceIdType.MESH,
        ).start()

    def arrived(view, link):
        pltpu.make_async_copy(view, view, recv.at[link]).wait()

    def left(view, link):
        pltpu.make_async_copy(view, view, send.at[link]).wait()

    pending = []

    def share_parts(buffer):
        link = channel()
        own = buffer.at[me]
        each_part(lambda device: push(own, own, link, device))
        view = buffer.at[pl.ds(0, parts - 1)]
        pending.append((view, link))
        return lambda: arrived(view, link)

    def share_all(buffer):
        link = channel()
        own = buffer.at[place]

        each_device(lambda device: push(own, own, link, device))
        view = buffer.at[pl.ds(0, devices - 1)]
        pending.append((view, link))
        return lambda: arrived(view, link)

    barrier = pltpu.get_barrier_semaphore()

    def greet(device):
        pl.semaphore_signal(barrier, inc=1, device_id=device, device_id_type=pl.DeviceIdType.MESH)

    each_device(greet)

    alpha = [(2.0 * grid_ref[k].astype(F32) + (1.0 - GRID)) * (1.0 / GRID) for k in range(2)]

    def square_sum(value):
        return jnp.sum(value * value, axis=-1, keepdims=True)

    def pointwise_filters(base_ref, dir_ref, target, b):
        base, first, second = (v.astype(F32) for v in (base_ref[b], dir_ref[0, b], dir_ref[1, b]))
        norm = square_sum(base)
        target[b, me] = (
            base
            + alpha[0] * unit_ratio(norm, square_sum(first)) * first
            + alpha[1] * unit_ratio(norm, square_sum(second)) * second
        ).astype(BF16)

    def send_reduce(b):
        have[("r", b)] = share_parts(pr.at[b])

    def send_spatial(b):
        base, first, second = (v.astype(F32) for v in (ws_ref[b], ds_ref[0, b], ds_ref[1, b]))
        norm, norm_a, norm_b = (
            jnp.sum(square_sum(v), axis=0) for v in (base, first, second)
        )
        value = (
            base
            + (alpha[0] * unit_ratio(norm, norm_a))[None] * first
            + (alpha[1] * unit_ratio(norm, norm_b))[None] * second
        )
        ps[b, me] = jnp.concatenate([value[t] for t in range(value.shape[0])], axis=-1).astype(BF16)
        have[("s", b)] = share_parts(ps.at[b])

    def send_expand(b):
        pointwise_filters(we_ref, de_ref, pe, b)
        have[("e", b)] = share_parts(pe.at[b])

    def class_arrays():
        return [v.astype(F32) for v in (wc_ref[...], dc_ref[0], dc_ref[1])]

    def send_norms():
        nc[me] = jnp.concatenate(
            [jnp.sum(v * v, axis=0, keepdims=True) for v in class_arrays()], axis=0
        )
        have["norms"] = share_parts(nc)

    def send_class():
        have["norms"]()
        sums = jnp.sum(nc[...], axis=0)
        base_sq = sums[0:1]
        base, first, second = class_arrays()
        pc[me] = (
            base
            + alpha[0] * unit_ratio(base_sq, sums[1:2]) * first
            + alpha[1] * unit_ratio(base_sq, sums[2:3]) * second
        ).astype(BF16)
        have["class"] = share_parts(pc)

    def ready(kind, source, b):
        have[(kind, b)]()
        return rows_joined(source[b])

    have = {}
    pointwise_filters(wr_ref, dr_ref, pr, 0)
    pl.semaphore_wait(barrier, devices - 1)
    send_reduce(0)
    send_spatial(0)
    send_expand(0)

    xs[...] = jnp.zeros_like(xs)
    xs[:, 0:cols, :] = x_ref[...]

    def inside(depth):
        return lax.broadcasted_iota(jnp.int32, (1, pitch, depth), 1) < cols

    edge_row = lax.broadcasted_iota(jnp.int32, (rows + 2, 1, mid), 0)
    edge_col = lax.broadcasted_iota(jnp.int32, (1, pitch, mid), 1)
    far_row = jnp.where(my_y == 0, rows + 1, 0)
    far_col = jnp.where(my_x == 0, cols, pitch - 1)
    valid = ((edge_row >= 1) & (edge_row <= rows) | (edge_row == far_row)) & (
        (edge_col < cols) | (edge_col == far_col)
    )
    near_row = jnp.where(my_y == 0, rows, 1)
    near_col = pl.multiple_of(jnp.where(my_x == 0, last, 0), 8)
    slot = far_col - last

    def local_stats(value):
        origin = value[0:1, 0:1, :]
        gap = jnp.where(inside(value.shape[-1]), value - origin, 0.0)
        offset = jnp.sum(gap, axis=(0, 1), keepdims=True)[0] / (rows * cols)
        square = jnp.sum(gap * gap, axis=(0, 1), keepdims=True)[0] / (rows * cols)
        return origin[0] + offset, jnp.maximum(square - offset * offset, 0.0)

    def pooled_stats(buffer, r):
        means, spreads = buffer[r, :, 0:1, :], buffer[r, :, 1:2, :]
        mean = jnp.mean(means, axis=0)
        gap = means - mean[None]
        return mean, jnp.mean(spreads, axis=0) + jnp.mean(gap * gap, axis=0)

    def batch_stats(value, alls, r, meanwhile):
        mean, var = local_stats(value)
        alls[r, place, 0:1, :] = mean
        alls[r, place, 1:2, :] = var
        come = share_all(alls.at[r])
        other = meanwhile()
        come()
        mean, var = pooled_stats(alls, r)
        return mean, lax.rsqrt(var + EPS_BN), other

    def after_first(b):
        if b == 0:
            send_norms()
        elif b == 1 and blocks > 1:
            send_class()
        return ready("s", ps, b)

    def after_second(b):
        if b + 1 < blocks:
            pointwise_filters(wr_ref, dr_ref, pr, b + 1)
            send_reduce(b + 1)
            send_spatial(b + 1)
        return ready("e", pe, b)

    def after_third(b):
        if b + 1 < blocks:
            send_expand(b + 1)
            return ready("r", pr, b + 1)
        if "class" not in have:
            send_class()
        return None

    w_reduce = ready("r", pr, 0)
    for b in range(blocks):
        y = lax.dot_general(
            xs[...].reshape(flat, width), w_reduce, NT, preferred_element_type=F32
        )
        edge[1 : rows + 1] = y.reshape(rows, pitch, mid)
        links = (channel(), channel(), channel())
        push(edge.at[near_row], halo_row.at[b], links[0], across)
        push(
            edge.at[pl.ds(1, rows), pl.ds(near_col, 8), :], halo_col.at[b], links[1], beside
        )
        push(edge.at[near_row, pl.ds(near_col, 8), :], halo_cor.at[b], links[2], corner)
        mean, scale, w = batch_stats(
            edge[1 : rows + 1], all_mid, 2 * b, functools.partial(after_first, b)
        )
        for view, link in zip((halo_row.at[b], halo_col.at[b], halo_cor.at[b]), links):
            left(view, link)
            arrived(view, link)
        shifted = pltpu.roll(halo_col[b].reshape(rows * 8, mid), 4, 0).reshape(rows, 8, mid)
        lane8 = lax.broadcasted_iota(jnp.int32, (1, 8, mid), 1)
        edge[1 : rows + 1, last:pitch, :] = jnp.where(
            lane8 == slot, shifted, edge[1 : rows + 1, last:pitch, :]
        )
        edge[far_row] = halo_row[b]
        end8 = lax.broadcasted_iota(jnp.int32, (8, mid), 0)
        edge[far_row, last:pitch, :] = jnp.where(
            end8 == slot, pltpu.roll(halo_cor[b], 4, 0), halo_row[b, last:pitch, :]
        )
        gain = scale * gm_ref[b, 0:1]
        a = jnp.where(
            valid,
            jax.nn.relu((edge[...] - mean[None]) * gain[None] + sm_ref[b, 0:1][None]),
            0.0,
        )
        tall = (rows + 2) * pitch
        prev = pltpu.roll(a, 1, 1).reshape(tall, mid)
        after = pltpu.roll(a, pitch - 1, 1).reshape(tall, mid)
        wide = jnp.concatenate([prev, a.reshape(tall, mid), after], axis=-1).astype(BF16)
        span = 3 * mid
        y = sum(
            lax.dot_general(
                wide[i * pitch : i * pitch + flat],
                w[:, i * span : (i + 1) * span],
                NT,
                preferred_element_type=F32,
            )
            for i in range(3)
        )
        y2s[...] = y.reshape(rows, pitch, mid)
        mean, scale, w = batch_stats(
            y2s[...], all_mid, 2 * b + 1, functools.partial(after_second, b)
        )
        gain = scale * gm_ref[b, 1:2]
        c = jax.nn.relu((y2s[...] - mean[None]) * gain[None] + sm_ref[b, 1:2][None])
        y = lax.dot_general(
            c.reshape(flat, mid).astype(BF16), w, NT, preferred_element_type=F32
        )
        y3s[...] = y.reshape(rows, pitch, width)
        mean, scale, w_reduce = batch_stats(
            y3s[...], all_out, b, functools.partial(after_third, b)
        )
        gain = scale * go_ref[b : b + 1]
        e = (y3s[...] - mean[None]) * gain[None] + so_ref[b : b + 1][None]
        xs[...] = jax.nn.relu(xs[...].astype(F32) + e).astype(BF16)

    final = jnp.where(inside(width), xs[...].astype(F32), 0.0)
    pooled_parts[place, 0:1, :] = jnp.sum(final, axis=(0, 1), keepdims=True)[0]
    pooled_parts[place, 1:2, :] = jnp.full((1, width), labels_ref[0].astype(F32))
    have_pooled = share_all(pooled_parts)
    out_ref[...] = xs[:, 0:cols, :]
    have["class"]()
    w = rows_joined(pc[...])
    have_pooled()
    by_image = [
        functools.reduce(jnp.add, [pooled_parts[i * tiles + t, 0:1, :] for t in range(tiles)])
        for i in range(parts)
    ]
    pooled = (jnp.concatenate(by_image, axis=0) / (rows * cols * tiles)).astype(BF16)
    wanted = jnp.concatenate([pooled_parts[i * tiles, 1:2, 0:1] for i in range(parts)], axis=0)
    logits = jnp.dot(pooled, w, preferred_element_type=F32)
    summed = jnp.log(jnp.sum(jnp.exp(logits), axis=1, keepdims=True))
    index = lax.broadcasted_iota(jnp.int32, logits.shape, 1).astype(F32)
    picked = jnp.sum(jnp.where(index == wanted, logits, 0.0), axis=1, keepdims=True)
    losses = summed - picked
    image = lax.broadcasted_iota(jnp.int32, losses.shape, 0)
    loss_ref[...] = jnp.broadcast_to(
        jnp.sum(jnp.where(image == me, losses, 0.0), axis=0, keepdims=True), loss_ref.shape
    )
    mean_ref[...] = jnp.broadcast_to(
        jnp.sum(losses, axis=0, keepdims=True) / parts, mean_ref.shape
    )
    for view, link in pending:
        left(view, link)


def fused(mesh, *args):
    (features, labels, grid, w_reduce, w_spatial, w_expand, w_class) = args[:7]
    (dir_reduce, dir_spatial, dir_expand, dir_class) = args[7:11]
    parts = mesh.shape["dp"]
    _, rows, cols, width = features.shape
    blocks, mid = w_expand.shape[0], w_expand.shape[1]
    taps = w_spatial.shape[1] * w_spatial.shape[2]
    own_mid, own_out = w_reduce.shape[-1], w_expand.shape[-1]
    own_feat, classes = w_class.shape
    pitch = round_up(cols + 2, 8)

    def spatial(v, lead):
        return jnp.swapaxes(v, -1, -2).reshape(lead + (taps, own_mid, mid))

    operands = (
        features[0],
        labels,
        grid,
        jnp.swapaxes(w_reduce, -1, -2),
        spatial(w_spatial, (blocks,)),
        jnp.swapaxes(w_expand, -1, -2),
        w_class,
        jnp.swapaxes(dir_reduce, -1, -2),
        spatial(dir_spatial, (2, blocks)),
        jnp.swapaxes(dir_expand, -1, -2),
        dir_class,
    ) + tuple(args[11:])
    vmem = pl.BlockSpec(memory_space=pltpu.VMEM)
    smem = pl.BlockSpec(memory_space=pltpu.SMEM)
    links = 3 + 9 * blocks
    out, loss, mean_loss = pl.pallas_call(
        functools.partial(section_kernel, parts),
        out_shape=(
            jax.ShapeDtypeStruct((rows, cols, width), BF16),
            jax.ShapeDtypeStruct((1, 128), F32),
            jax.ShapeDtypeStruct((1, 128), F32),
        ),
        in_specs=[vmem, smem, smem] + [vmem] * 12,
        out_specs=(vmem, vmem, vmem),
        scratch_shapes=[
            pltpu.VMEM((rows, pitch, width), BF16),
            pltpu.VMEM((rows + 2, pitch, mid), F32),
            pltpu.VMEM((rows, pitch, mid), F32),
            pltpu.VMEM((rows, pitch, width), F32),
            pltpu.VMEM((blocks, parts, own_mid, width), BF16),
            pltpu.VMEM((blocks, parts, own_mid, taps * mid), BF16),
            pltpu.VMEM((blocks, parts, own_out, mid), BF16),
            pltpu.VMEM((parts, own_feat, classes), BF16),
            pltpu.VMEM((parts, 3, classes), F32),
            pltpu.VMEM((2 * blocks, parts * 4, 2, mid), F32),
            pltpu.VMEM((blocks, parts * 4, 2, width), F32),
            pltpu.VMEM((blocks, pitch, mid), F32),
            pltpu.VMEM((blocks, rows, 8, mid), F32),
            pltpu.VMEM((blocks, 8, mid), F32),
            pltpu.VMEM((parts * 4, 2, width), F32),
            pltpu.SemaphoreType.DMA((links,)),
            pltpu.SemaphoreType.DMA((links,)),
        ],
        compiler_params=pltpu.CompilerParams(
            collective_id=0, has_side_effects=True, vmem_limit_bytes=56 * 2**20
        ),
    )(*operands)
    return out[None], loss[0, 0:1], mean_loss[0, 0]


def body(mesh, *args):
    features = args[0]
    plain = mesh.shape["sy"] == 2 and mesh.shape["sx"] == 2 and mesh.shape["dp"] > 1
    if plain and features.shape[0] == 1 and features.shape[2] % 8 == 4:
        return fused(mesh, *args)
    return per_device(*args)


def solution(mesh):
    in_specs = (
        P("dp", "sy", "sx", None),
        P("dp"),
        P(),
        P(None, None, "dp"),
        P(None, None, None, None, "dp"),
        P(None, None, "dp"),
        P("dp", None),
        P(None, None, None, "dp"),
        P(None, None, None, None, None, "dp"),
        P(None, None, None, "dp"),
        P(None, "dp", None),
        P(),
        P(),
        P(),
        P(),
    )
    out_specs = (P("dp", "sy", "sx", None), P("dp"), P())
    return jax.shard_map(
        functools.partial(body, mesh), mesh=mesh, in_specs=in_specs, out_specs=out_specs, check_vma=False
    )
```
